32 devices in a mesh: row: 8 (over z, core), col: 4 (over y, x).
Axes of the slice: x: 2, y: 2, z: 4, core: 2. Of those that a mesh axis runs over, the one named last changes fastest.
Arguments:
- velocity: float32 [1, 3, 64, 64, 256], P(None, None, 'row', 'col'), may hold values from -6 to 6
- tendency: float32 [1, 3, 64, 64, 256], P(None, None, 'row', 'col'), may hold values from -6 to 6
- step_size: float32 [1], replicated, may hold values from 0.1 to 0.6
- lift_weight: float32 [32, 3], replicated, may hold values from -3.5 to 3.5
- lift_bias: float32 [32], replicated, may hold values from -3 to 3
- spectral_weight: bfloat16 [2, 32, 32, 32, 1024], P(None, 'row', 'col'), may hold values from -6 to 6
- local_weight: float32 [32, 32], replicated, may hold values from -1 to 1
- local_bias: float32 [32], replicated, may hold values from -3 to 3
Outputs:
- features: bfloat16 [1, 32, 64, 64, 256], P(None, None, 'row', 'col')
The draws below stay inside these ranges and needn't reach their ends.
All inputs are finite; a program needn't handle non-finite values.
Results may differ from the reference program's by a relative error of at most 0.001.
Values sent between devices are 32-bit elements; how exact they have to be, the bound alone decides.
A program may use at most 64 MiB of HBM per device.

```python
import math
import jax
import jax.numpy as jnp
from jax import lax

CHANNELS = 32
KX = 32
KY = 32
KZ = 32
NZ = 256
SAMPLES = 1
NX = 64
NY = 64


def block_levels(key, dims, shards, low, high):
    factor_of, own = 1.0, jax.random.fold_in(key, 6)
    for position, shards_of in shards:
        heights = jnp.exp(jax.random.uniform(jax.random.fold_in(own, position), (shards_of,), jnp.float32, low / len(shards), high / len(shards)))
        factor_of = factor_of * jnp.repeat(heights, dims[position] // shards_of).reshape([-1 if axis == position else 1 for axis in range(len(dims))])
    return factor_of


def centred(key, dims, scale, reach, pieces=(), kind=jnp.bfloat16):
    gain = block_levels(key, dims, pieces, -0.22, 0.18) if pieces else 1.0
    entries = jax.random.normal(key, dims, jnp.float32) * scale * gain
    return jnp.minimum(jnp.maximum(entries, -reach), reach).astype(kind)


def setup_inputs(seed: int = 0) -> dict:
    arg_keys = jax.random.split(jax.random.key(seed), 9)
    velocity = centred(arg_keys[0], (SAMPLES, 3, NX, NY, NZ), 1.0, 6.0, ((2, 8), (3, 4)), jnp.float32)
    tendency = centred(arg_keys[1], (SAMPLES, 3, NX, NY, NZ), 1.0, 6.0, ((2, 8), (3, 4)), jnp.float32)
    step_size = jnp.clip(jnp.exp(jax.random.uniform(arg_keys[2], (SAMPLES,), jnp.float32, math.log(0.1), math.log(0.6))), 0.1, 0.6)
    lift_weight = centred(arg_keys[3], (CHANNELS, 3), 3 ** -0.5, 3.5, (), jnp.float32)
    lift_bias = centred(arg_keys[4], (CHANNELS,), 0.5, 3.0, (), jnp.float32)
    spectral_weight = centred(arg_keys[5], (2, KY, KZ, KX, CHANNELS * CHANNELS), 1.0, 6.0, ((1, 8), (2, 4)))
    local_weight = centred(arg_keys[6], (CHANNELS, CHANNELS), CHANNELS ** -0.5, 1.0, (), jnp.float32)
    local_bias = centred(arg_keys[7], (CHANNELS,), 0.5, 3.0, (), jnp.float32)
    return dict(velocity=velocity, tendency=tendency, step_size=step_size, lift_weight=lift_weight, lift_bias=lift_bias, spectral_weight=spectral_weight, local_weight=local_weight, local_bias=local_bias)


def positions(count, length):
    index = jnp.arange(count, dtype=jnp.int32)
    return jnp.where(index < count // 2, index, length - count + index).astype(jnp.int32)


def reference(velocity, tendency, step_size, lift_weight, lift_bias, spectral_weight, local_weight, local_bias):
    highest = lax.Precision.HIGHEST
    x_pos = positions(KX, NX)
    y_pos = positions(KY, NY)
    z_pos = jnp.arange(KZ, dtype=jnp.int32)
    volume = NX * NY * NZ
    weights = spectral_weight.astype(jnp.float32).reshape(2, KY, KZ, KX, CHANNELS, CHANNELS)
    complex_weights = weights[0] + 1j * weights[1]
    combined = jnp.dot(local_weight, lift_weight, precision=highest)
    offset = jnp.dot(local_weight, lift_bias, precision=highest) + local_bias
    results = []
    for sample in range(SAMPLES):
        advanced = velocity[sample] + step_size[sample] * tendency[sample]

        def forward(channel):
            lifted = (lift_weight[channel, 0] * advanced[0] + lift_weight[channel, 1] * advanced[1]
                      + lift_weight[channel, 2] * advanced[2] + lift_bias[channel])
            spectrum = jnp.fft.rfftn(lifted)
            kept = spectrum[x_pos][:, y_pos][:, :, :KZ]
            return kept / volume

        coeffs = lax.map(forward, jnp.arange(CHANNELS, dtype=jnp.int32))
        mixed = jnp.einsum("egaoi,iaeg->oaeg", complex_weights, coeffs, precision=highest)

        def inverse(channel):
            full = jnp.zeros((NX, NY, NZ // 2 + 1), mixed.dtype)
            full = full.at[x_pos[:, None, None], y_pos[None, :, None], z_pos[None, None, :]].set(mixed[channel])
            spectral = jnp.fft.irfftn(full, s=(NX, NY, NZ)) * volume
            local = (combined[channel, 0] * advanced[0] + combined[channel, 1] * advanced[1]
                     + combined[channel, 2] * advanced[2] + offset[channel])
            return jax.nn.gelu(spectral + local).astype(jnp.bfloat16)

        results.append(lax.map(inverse, jnp.arange(CHANNELS, dtype=jnp.int32)))
    return jnp.stack(results, 0)
```

```python
import functools
import math

import jax
import jax.numpy as jnp
import numpy as np
from jax import lax
from jax.experimental import pallas as pl
from jax.experimental.pallas import tpu as pltpu
from jax.sharding import PartitionSpec as P

KX = 32
KY = 32
KZ = 32
HIGHEST = lax.Precision.HIGHEST
F32 = jnp.float32
BF16 = jnp.bfloat16


def waves(count):
    index = np.arange(count)
    return np.where(index < count // 2, index, index - count)


def trig(wave, length):
    angle = ((wave[:, None] * np.arange(length)[None, :]) % length) * (2.0 * math.pi / length)
    return np.cos(angle), np.sin(angle)


def np_halves(table):
    table = np.asarray(table, np.float32)
    high = table.astype(jnp.bfloat16)
    low = (table - high.astype(np.float32)).astype(jnp.bfloat16)
    return high, low


def split(x):
    high = x.astype(BF16)
    return high, (x - high.astype(F32)).astype(BF16)


def dot(a, b):
    return jnp.dot(a, b, preferred_element_type=F32)


def mix_kernel(kyl, kzl, scale, u_ref, wl_ref, xf_ref, selc_ref, sels_ref, flag_ref, xb_ref, out_ref, m_ref):
    sources, rows, wide = u_ref.shape
    a = rows // kyl
    cos_parts, sin_parts = [], []
    for l in range(kyl):
        u = u_ref[:, l * a:(l + 1) * a, :].reshape(sources * a, wide)
        q = jnp.dot(xf_ref[...], u, precision=HIGHEST, preferred_element_type=F32) * scale
        cos_parts.append(q[:KX])
        sin_parts.append(q[KX:])
    ch, cl = split(jnp.concatenate(cos_parts, 0))
    sh, sl = split(jnp.concatenate(sin_parts, 0))
    selc, sels = selc_ref[...], sels_ref[...]
    amp = dot(ch, selc) + dot(cl, selc) + dot(sh, sels) + dot(sl, sels)
    lane = lax.broadcasted_iota(jnp.int32, (KX, 128), 1)
    row = lax.broadcasted_iota(jnp.int32, (KX, 128), 0)
    quarter = lane // 32
    for group in range(kyl * kzl // 4):
        packed_r = packed_i = None
        for q in range(4):
            l, k = divmod(group * 4 + q, kzl)
            ar = amp[l * KX:(l + 1) * KX, k * 256:k * 256 + 128]
            ai = amp[l * KX:(l + 1) * KX, k * 256 + 128:k * 256 + 256]
            if l == 0 and k == 0:
                ar = ar + jnp.where(row == 0, flag_ref[...], 0.0)
            at = pl.ds((l * kzl + k) * KX, KX)
            wr = wl_ref[0, at, :128] + wl_ref[0, at, 128:]
            wi = wl_ref[1, at, :128] + wl_ref[1, at, 128:]
            pr = wr * ar - wi * ai
            pi = wr * ai + wi * ar
            pr = pr + pltpu.roll(pr, 64, 1)
            pi = pi + pltpu.roll(pi, 64, 1)
            pr = pr + pltpu.roll(pr, 32, 1)
            pi = pi + pltpu.roll(pi, 32, 1)
            packed_r = pr if q == 0 else jnp.where(quarter == q, pr, packed_r)
            packed_i = pi if q == 0 else jnp.where(quarter == q, pi, packed_i)
        cols = slice(group * 128, (group + 1) * 128)
        m = jnp.concatenate([packed_r, packed_i], 0)
        mh, ml = split(m)
        m_ref[0:2 * KX, cols] = mh
        m_ref[2 * KX:4 * KX, cols] = ml
        m_ref[4 * KX:6 * KX, cols] = mh
    back = dot(xb_ref[...], m_ref[...])
    out_ref[...] = back.reshape(out_ref.shape)


def y_back_kernel(kyl, d_ref, yh_ref, yl_ref, out_ref, lhs_ref):
    total = d_ref.shape[0]
    ko = d_ref.shape[1] // kyl
    count, halves_v, _, cells = out_ref.shape
    pairs = yh_ref.shape[1]
    a = total // pairs
    for l in range(kyl):
        t = jnp.transpose(d_ref[:, l * ko:(l + 1) * ko])
        th, tl = split(t)
        lhs_ref[:, l * total:(l + 1) * total] = th
        lhs_ref[:, (kyl + l) * total:(kyl + l + 1) * total] = tl
        lhs_ref[:, (2 * kyl + l) * total:(2 * kyl + l + 1) * total] = th
    width = halves_v * cells
    b = cells // a
    xr = lax.broadcasted_iota(jnp.int32, (pairs, a, width), 1)
    xl = (lax.broadcasted_iota(jnp.int32, (pairs, a, width), 2) // b) % a
    same = xr == xl

    def expand(table):
        full = jnp.where(same, table.astype(F32)[:, None, :], 0.0)
        return full.reshape(total, width).astype(BF16)

    for d in range(count):
        cols = slice(d * width, (d + 1) * width)
        high = [expand(yh_ref[l, :, cols]) for l in range(kyl)]
        low = [expand(yl_ref[l, :, cols]) for l in range(kyl)]
        rhs = jnp.concatenate(high + high + low, 0)
        acc = dot(lhs_ref[...], rhs)
        for v in range(halves_v):
            out_ref[d, v] = acc[:, v * cells:(v + 1) * cells]


def z_back_kernel(channels, block, d_ref, vel_ref, tend_ref, step_ref, comb_ref, off_ref, tz_ref, out_ref, adv_ref):
    first = pl.program_id(0)
    depth = d_ref.shape[0] // channels

    @pl.when(first == 0)
    def _():
        adv_ref[...] = vel_ref[...] + step_ref[0] * tend_ref[...]

    for i in range(block):
        o = first * block + i
        high, low = split(d_ref[pl.ds(o, depth, stride=channels), :])
        lhs = jnp.concatenate([high, low, high], 0)
        spectral = lax.dot_general(lhs, tz_ref[...], (((0,), (0,)), ((), ())), preferred_element_type=F32)
        x = spectral + off_ref[o]
        for j in range(adv_ref.shape[0]):
            x = x + comb_ref[o, j] * adv_ref[j]
        inner = x * (0.7978845608028654 + 0.035677408136300125 * (x * x))
        half = 0.5 * x
        out_ref[i] = (half + half * jnp.tanh(inner)).astype(BF16)


def per_device(
    velocity, tendency, step_size, lift_weight, lift_bias, spectral_weight, local_weight, local_bias
):
    samples, width_in, a, b, nz = velocity.shape
    channels = lift_weight.shape[0]
    rows, cols = lax.axis_size("row"), lax.axis_size("col")
    full_x, full_y = a * rows, b * cols
    kzl, kyl = KZ // cols, KY // rows
    modes = kyl * kzl * KX
    cells = a * b
    vmem = pl.BlockSpec(memory_space=pltpu.VMEM)
    smem = pl.BlockSpec(memory_space=pltpu.SMEM)
    big = pltpu.CompilerParams(vmem_limit_bytes=48 * 1024 * 1024)

    lift4 = jnp.concatenate([lift_weight, lift_bias[:, None]], 1)
    group = width_in + 1
    eye = jnp.eye(channels, dtype=F32)
    lift_lanes = jnp.repeat(lift4, channels, axis=1)
    lift_full = jnp.tile(lift_lanes, (channels, 1))
    own = jnp.tile(jnp.repeat(eye, channels, axis=0), (1, group))
    masked = lift_full * own
    high = lax.reduce_precision(masked, 8, 7)
    lh, ll = high.astype(BF16), (masked - high).astype(BF16)
    stored = spectral_weight.reshape(2 * modes, channels * channels)
    lifted_weight = dot(stored, jnp.concatenate([lh, ll], 1)).reshape(2, modes, 2 * group * channels)

    zc, zs = trig(np.arange(KZ), nz)
    zf = np.stack([zc, -zs], 0).reshape(2, cols, kzl, nz).transpose(1, 0, 2, 3).reshape(2 * KZ, nz)
    yc, ys = trig(waves(KY), full_y)
    xc, xs = trig(waves(KX), full_x)
    xf = np.concatenate([xc, xs], 0).astype(np.float32)
    selc = np.zeros((2, width_in, kzl, kzl, 2, group, channels), np.float32)
    sels = np.zeros_like(selc)
    for j in range(width_in):
        for k in range(kzl):
            selc[0, j, k, k, 0, j] = 1
            selc[1, j, k, k, 1, j] = 1
            sels[1, j, k, k, 0, j] = 1
            sels[0, j, k, k, 1, j] = -1
    wide = 2 * width_in * kzl
    selc = selc.reshape(wide, -1)
    sels = sels.reshape(wide, -1)
    xb = np.stack([np.stack([xc, -xs], 0), np.stack([xs, xc], 0)], 0)
    xb = xb.reshape(2, 2, KX, rows, a).transpose(3, 0, 4, 1, 2).reshape(rows * 2 * a, 2 * KX)
    xbh, xbl = np_halves(xb)
    xb3 = np.concatenate([xbh, xbh, xbl], 1)
    yb = np.stack([np.stack([yc, ys], 0), np.stack([-ys, yc], 0)], 0)
    yb = yb.reshape(2, 2, rows, kyl, cols, b).transpose(3, 2, 0, 4, 1, 5)
    yb = np.broadcast_to(yb[:, :, :, :, :, None, :], (kyl, rows, 2, cols, 2, a, b)).reshape(kyl, rows * 2, cols * 2 * cells)
    ybh, ybl = np_halves(yb)
    twice = np.where(np.arange(KZ) == 0, 1.0, 2.0)[:, None]
    zb = np.stack([twice * zc, -twice * zs], 0).reshape(2, cols, kzl, nz).transpose(1, 0, 2, 3).reshape(2 * KZ, nz)
    zbh, zbl = np_halves(zb)
    zb3 = np.concatenate([zbh, zbh, zbl], 0)
    yf = np.stack([yc, ys], 0).reshape(2, rows, kyl, 1, cols, 1, b)
    yf = (yf * np.eye(a).reshape(1, 1, 1, a, 1, a, 1)).reshape(2, rows * kyl * a, cols, cells)

    combined = jnp.dot(local_weight, lift_weight, precision=HIGHEST)
    offset = jnp.dot(local_weight, lift_bias, precision=HIGHEST) + local_bias
    origin = (lax.axis_index("row") == 0) & (lax.axis_index("col") == 0)
    last = np.arange(group * channels)[None, :] >= width_in * channels
    flag = jnp.where(jnp.asarray(last) & origin, 1.0, 0.0).astype(F32)

    results = []
    for sample in range(samples):
        vel = velocity[sample].reshape(width_in * cells, nz)
        tend = tendency[sample].reshape(width_in * cells, nz)
        step = step_size[sample]
        advanced = vel + step * tend
        z_modes = lax.dot_general(jnp.asarray(zf, F32), advanced, (((1,), (1,)), ((), ())), precision=HIGHEST)
        arrived = lax.all_to_all(z_modes.reshape(cols, 2 * kzl, width_in * cells), "col", 0, 0, tiled=True)
        arrived = arrived.reshape(cols, 2, kzl, width_in, cells)
        by_y = jnp.einsum("pgsn,srkjn->pgrjk", jnp.asarray(yf, F32), arrived, precision=HIGHEST)
        real = by_y[0, :, 0] + by_y[1, :, 1]
        imag = by_y[0, :, 1] - by_y[1, :, 0]
        by_y = jnp.stack([real, imag], 1).reshape(rows, kyl * a, wide)
        pencils_x = lax.all_to_all(by_y, "row", 0, 0, tiled=True)
        cells_x = pl.pallas_call(
            functools.partial(mix_kernel, kyl, kzl, 1.0 / (full_x * full_y * nz)),
            out_shape=jax.ShapeDtypeStruct((rows, 2 * a, kyl * kzl * channels), F32),
            in_specs=[vmem] * 7,
            out_specs=vmem,
            scratch_shapes=[pltpu.VMEM((6 * KX, kyl * kzl * channels), BF16)],
            compiler_params=big,
        )(pencils_x, lifted_weight, jnp.asarray(xf), jnp.asarray(selc, BF16), jnp.asarray(sels, BF16), flag, jnp.asarray(xb3))
        by_cells = lax.all_to_all(cells_x, "row", 0, 0, tiled=True)
        by_cells = by_cells.reshape(rows * 2 * a, kyl * kzl * channels)
        cells_y = pl.pallas_call(
            functools.partial(y_back_kernel, kyl),
            out_shape=jax.ShapeDtypeStruct((cols, 2, kzl * channels, cells), F32),
            in_specs=[vmem] * 3,
            out_specs=vmem,
            scratch_shapes=[pltpu.VMEM((kzl * channels, 3 * kyl * rows * 2 * a), BF16)],
            compiler_params=big,
        )(by_cells, jnp.asarray(ybh), jnp.asarray(ybl))
        pencils_z = lax.all_to_all(cells_y, "col", 0, 0, tiled=True).reshape(cols * 2 * kzl * channels, cells)
        block = 4
        whole = lambda *shape: pl.BlockSpec(shape, lambda i: (0,) * len(shape))
        features = pl.pallas_call(
            functools.partial(z_back_kernel, channels, block),
            grid=(channels // block,),
            out_shape=jax.ShapeDtypeStruct((channels, cells, nz), BF16),
            in_specs=[
                whole(*pencils_z.shape), whole(width_in, cells, nz), whole(width_in, cells, nz),
                smem, smem, smem, whole(*zb3.shape),
            ],
            out_specs=pl.BlockSpec((block, cells, nz), lambda i: (i, 0, 0)),
            scratch_shapes=[pltpu.VMEM((width_in, cells, nz), F32)],
            compiler_params=big,
        )(
            pencils_z, vel.reshape(width_in, cells, nz), tend.reshape(width_in, cells, nz),
            step.reshape(1), combined, offset, jnp.asarray(zb3),
        )
        results.append(features.reshape(channels, a, b, nz))
    return jnp.stack(results, 0)


def solution(mesh):
    in_specs = (
        P(None, None, "row", "col", None),
        P(None, None, "row", "col", None),
        P(),
        P(),
        P(),
        P(None, "row", "col", None, None),
        P(),
        P(),
    )
    out_specs = P(None, None, "row", "col", None)
    return jax.shard_map(
        per_device, mesh=mesh, in_specs=in_specs, out_specs=out_specs, check_vma=False
    )
```

```python
import functools
import math

import jax
import jax.numpy as jnp
import numpy as np
from jax import lax
from jax.experimental import pallas as pl
from jax.experimental.pallas import tpu as pltpu
from jax.sharding import PartitionSpec as P

KX = 32
KY = 32
KZ = 32
HIGHEST = lax.Precision.HIGHEST
F32 = jnp.float32
BF16 = jnp.bfloat16


def waves(count):
    index = np.arange(count)
    return np.where(index < count // 2, index, index - count)


def trig(wave, length):
    angle = ((wave[:, None] * np.arange(length)[None, :]) % length) * (2.0 * math.pi / length)
    return np.cos(angle), np.sin(angle)


def np_halves(table):
    table = np.asarray(table, np.float32)
    high = table.astype(jnp.bfloat16)
    low = (table - high.astype(np.float32)).astype(jnp.bfloat16)
    return high, low


def split(x):
    high = x.astype(BF16)
    return high, (x - high.astype(F32)).astype(BF16)


def dot(a, b):
    return jnp.dot(a, b, preferred_element_type=F32)


MESH = pl.DeviceIdType.MESH


def layer_kernel(
    kyl, kzl, part, scale, vel_ref, tend_ref, step_ref, zf_ref, yfh_ref, yfl_ref, w_ref, lift_ref, xf_ref, selc_ref,
    sels_ref, flag_ref, xb_ref, yh_ref, yl_ref, out_ref, w_vmem, wl_ref, zsend, zrecv, ypad, ysend, yrecv, m_ref, xsend, xrecv,
    lhs_ref, csend, w_sem, z_ss, z_rs, y_ss, y_rs, x_ss, x_rs, c_ss, c_rs,
):
    rows, cols = lax.axis_size("row"), lax.axis_size("col")
    my_row, my_col = lax.axis_index("row"), lax.axis_index("col")
    width_in, cells, _ = vel_ref.shape
    rk = zf_ref.shape[0] // cols
    a = ysend.shape[1] // kyl
    b = cells // a
    modes = kyl * kzl * KX
    chunks = xsend.shape[0]

    load = pltpu.make_async_copy(w_ref, w_vmem, w_sem)
    load.start()
    barrier = pltpu.get_barrier_semaphore()
    row_peers = [lax.rem(my_row + i, rows) for i in range(1, rows)]
    col_peers = [lax.rem(my_col + i, cols) for i in range(1, cols)]
    for peer in row_peers:
        pl.semaphore_signal(barrier, inc=1, device_id={"row": peer}, device_id_type=MESH)
    for peer in col_peers:
        pl.semaphore_signal(barrier, inc=1, device_id={"col": peer}, device_id_type=MESH)

    for j in range(width_in):
        adv = vel_ref[j] + step_ref[0] * tend_ref[j]
        z = lax.dot_general(
            zf_ref[...], adv, (((1,), (1,)), ((), ())), precision=HIGHEST, preferred_element_type=F32
        )
        zsend[:, j * rk:(j + 1) * rk, :] = z.reshape(cols, rk, cells)
    pl.semaphore_wait(barrier, rows + cols - 2)
    z_copies = []
    for i, peer in enumerate(col_peers):
        copy = pltpu.make_async_remote_copy(
            zsend.at[peer], zrecv.at[my_col], z_ss.at[i], z_rs.at[i], device_id={"col": peer}, device_id_type=MESH
        )
        copy.start()
        z_copies.append(copy)
    zrecv[pl.ds(my_col, 1)] = zsend[pl.ds(my_col, 1)]

    load.wait()
    step_rows = modes // 2
    half_lanes = lift_ref.shape[1] // 2

    def weigh(n):
        at = slice(n * step_rows, (n + 1) * step_rows)
        both = dot(w_vmem[at, :], lift_ref[...])
        wl_ref[at, :] = both[:, :half_lanes] + both[:, half_lanes:]

    weigh(0)
    weigh(1)
    for copy in z_copies:
        copy.wait_recv()

    x = jnp.concatenate([zrecv[s] for s in range(cols)], 1)
    xh, xl = split(x)
    y = dot(xh, yfh_ref[...]) + dot(xl, yfh_ref[...]) + dot(xh, yfl_ref[...])
    lanes = rows * kyl * a
    ypad[...] = jnp.zeros_like(ypad)
    low_rows = lax.broadcasted_iota(jnp.int32, (rk, lanes), 0) < rk // 2
    for j in range(width_in):
        block = y[j * rk:(j + 1) * rk]
        turned = pltpu.roll(block[:, lanes:], rk // 2, 0)
        ypad[j * rk:(j + 1) * rk, :] = block[:, :lanes] + jnp.where(low_rows, turned, -turned)
    ysend[...] = jnp.transpose(ypad[...]).reshape(ysend.shape)
    y_copies = []
    for i, peer in enumerate(row_peers):
        copy = pltpu.make_async_remote_copy(
            ysend.at[peer], yrecv.at[my_row], y_ss.at[i], y_rs.at[i], device_id={"row": peer}, device_id_type=MESH
        )
        copy.start()
        y_copies.append(copy)
    yrecv[pl.ds(my_row, 1)] = ysend[pl.ds(my_row, 1)]
    weigh(2)
    weigh(3)
    for copy in y_copies:
        copy.wait_recv()

    cos_parts, sin_parts = [], []
    for l in range(kyl):
        u = yrecv[:, l * a:(l + 1) * a, :].reshape(rows * a, yrecv.shape[2])
        q = jnp.dot(xf_ref[...], u, precision=HIGHEST, preferred_element_type=F32) * scale
        cos_parts.append(q[:KX])
        sin_parts.append(q[KX:])
    ch, cl = split(jnp.concatenate(cos_parts, 0))
    sh, sl = split(jnp.concatenate(sin_parts, 0))
    selc, sels = selc_ref[...], sels_ref[...]
    amp = dot(ch, selc) + dot(cl, selc) + dot(sh, sels) + dot(sl, sels)
    lane = lax.broadcasted_iota(jnp.int32, (KX, 128), 1)
    row = lax.broadcasted_iota(jnp.int32, (KX, 128), 0)
    quarter = lane // 32
    order = [(l, c * part + k) for c in range(chunks) for l in range(kyl) for k in range(part)]
    chunk_lanes = xsend.shape[3]
    x_copies = []
    for c in range(chunks):
        for group in range(chunk_lanes // 128):
            packed_r = packed_i = None
            for q in range(4):
                l, k = order[(c * chunk_lanes // 128 + group) * 4 + q]
                ar = amp[l * KX:(l + 1) * KX, k * 256:k * 256 + 128]
                ai = amp[l * KX:(l + 1) * KX, k * 256 + 128:k * 256 + 256]
                if l == 0 and k == 0:
                    ar = ar + jnp.where(row == 0, flag_ref[...], 0.0)
                at = (l * kzl + k) * KX
                wr = wl_ref[at:at + KX, :]
                wi = wl_ref[modes + at:modes + at + KX, :]
                pr = wr * ar - wi * ai
                pi = wr * ai + wi * ar
                pr = pr + pltpu.roll(pr, 64, 1)
                pi = pi + pltpu.roll(pi, 64, 1)
                pr = pr + pltpu.roll(pr, 32, 1)
                pi = pi + pltpu.roll(pi, 32, 1)
                packed_r = pr if q == 0 else jnp.where(quarter == q, pr, packed_r)
                packed_i = pi if q == 0 else jnp.where(quarter == q, pi, packed_i)
            at = slice(group * 128, (group + 1) * 128)
            mh, ml = split(jnp.concatenate([packed_r, packed_i], 0))
            m_ref[0:2 * KX, at] = mh
            m_ref[2 * KX:4 * KX, at] = ml
            m_ref[4 * KX:6 * KX, at] = mh
        xsend[c] = dot(xb_ref[...], m_ref[...]).reshape(xsend.shape[1:])
        started = []
        for i, peer in enumerate(row_peers):
            copy = pltpu.make_async_remote_copy(
                xsend.at[c, peer], xrecv.at[c, my_row], x_ss.at[c, i], x_rs.at[c, i],
                device_id={"row": peer}, device_id_type=MESH,
            )
            copy.start()
            started.append(copy)
        xrecv[c, pl.ds(my_row, 1)] = xsend[c, pl.ds(my_row, 1)]
        x_copies.append(started)

    total = rows * 2 * a
    ko = chunk_lanes // kyl
    pairs = 2 * rows
    width = 2 * cells
    xr = lax.broadcasted_iota(jnp.int32, (pairs, a, width), 1)
    xl = (lax.broadcasted_iota(jnp.int32, (pairs, a, width), 2) // b) % a
    same = xr == xl

    def expand(table):
        full = jnp.where(same, table.astype(F32)[:, None, :], 0.0)
        return full.reshape(total, width).astype(BF16)

    c_copies = []
    for c in range(chunks):
        for copy in x_copies[c]:
            copy.wait_recv()
        for l in range(kyl):
            held = xrecv[c, :, :, l * ko:(l + 1) * ko].reshape(total, ko)
            th, tl = split(jnp.transpose(held))
            lhs_ref[:, l * total:(l + 1) * total] = th
            lhs_ref[:, (kyl + l) * total:(kyl + l + 1) * total] = tl
            lhs_ref[:, (2 * kyl + l) * total:(2 * kyl + l + 1) * total] = th
        at = pl.ds(c * ko, ko)
        for i in list(range(1, cols)) + [0]:
            d = lax.rem(my_col + i, cols)
            high = [expand(yh_ref[d, l]) for l in range(kyl)]
            low = [expand(yl_ref[d, l]) for l in range(kyl)]
            acc = dot(lhs_ref[...], jnp.concatenate(high + high + low, 0))
            if i == 0:
                for v in range(2):
                    out_ref[pl.ds(my_col, 1), v, at, :] = acc[:, v * cells:(v + 1) * cells][None]
            else:
                for v in range(2):
                    csend[c, i - 1, v] = acc[:, v * cells:(v + 1) * cells]
                copy = pltpu.make_async_remote_copy(
                    csend.at[c, i - 1], out_ref.at[my_col, :, at, :], c_ss.at[c, i - 1], c_rs.at[c, i - 1],
                    device_id={"col": d}, device_id_type=MESH,
                )
                copy.start()
                c_copies.append(copy)
    for copy in c_copies:
        copy.wait_recv()
    for copy in z_copies + y_copies + [copy for started in x_copies for copy in started] + c_copies:
        copy.wait_send()


def z_back_kernel(channels, block, d_ref, vel_ref, tend_ref, step_ref, comb_ref, off_ref, tz_ref, out_ref, adv_ref):
    first = pl.program_id(0)
    depth = d_ref.shape[0] // channels

    @pl.when(first == 0)
    def _():
        adv_ref[...] = vel_ref[...] + step_ref[0] * tend_ref[...]

    for i in range(block):
        o = first * block + i
        high, low = split(d_ref[pl.ds(o, depth, stride=channels), :])
        lhs = jnp.concatenate([high, low, high], 0)
        spectral = lax.dot_general(lhs, tz_ref[...], (((0,), (0,)), ((), ())), preferred_element_type=F32)
        x = spectral + off_ref[o]
        for j in range(adv_ref.shape[0]):
            x = x + comb_ref[o, j] * adv_ref[j]
        inner = x * (0.7978845608028654 + 0.035677408136300125 * (x * x))
        half = 0.5 * x
        out_ref[i] = (half + half * jnp.tanh(inner)).astype(BF16)


def per_device(
    velocity, tendency, step_size, lift_weight, lift_bias, spectral_weight, local_weight, local_bias
):
    samples, width_in, a, b, nz = velocity.shape
    channels = lift_weight.shape[0]
    rows, cols = lax.axis_size("row"), lax.axis_size("col")
    full_x, full_y = a * rows, b * cols
    kzl, kyl = KZ // cols, KY // rows
    modes = kyl * kzl * KX
    cells = a * b
    vmem = pl.BlockSpec(memory_space=pltpu.VMEM)
    smem = pl.BlockSpec(memory_space=pltpu.SMEM)
    big = pltpu.CompilerParams(vmem_limit_bytes=48 * 1024 * 1024)

    lift4 = jnp.concatenate([lift_weight, lift_bias[:, None]], 1)
    group = width_in + 1
    eye = jnp.eye(channels, dtype=F32)
    lift_lanes = jnp.repeat(lift4, channels, axis=1)
    lift_full = jnp.tile(lift_lanes, (channels, 1))
    own = jnp.tile(jnp.repeat(eye, channels, axis=0), (1, group))
    masked = lift_full * own
    high = lax.reduce_precision(masked, 8, 7)
    lh, ll = high.astype(BF16), (masked - high).astype(BF16)
    lift_map = jnp.concatenate([lh, ll], 1)
    stored = spectral_weight.reshape(2 * modes, channels * channels)

    zc, zs = trig(np.arange(KZ), nz)
    rk = 2 * max(kzl, 4)
    zf = np.zeros((cols, 2, rk // 2, nz), np.float32)
    zf[:, :, :kzl] = np.stack([zc, -zs], 0).reshape(2, cols, kzl, nz).transpose(1, 0, 2, 3)
    zf = zf.reshape(cols * rk, nz)
    yc, ys = trig(waves(KY), full_y)
    xc, xs = trig(waves(KX), full_x)
    xf = np.concatenate([xc, xs], 0).astype(np.float32)
    selc = np.zeros((128, kzl, 2, group, channels), np.float32)
    sels = np.zeros_like(selc)
    for j in range(width_in):
        for k in range(kzl):
            re, im = j * rk + k, j * rk + rk // 2 + k
            selc[re, k, 0, j] = 1
            selc[im, k, 1, j] = 1
            sels[im, k, 0, j] = 1
            sels[re, k, 1, j] = -1
    selc = selc.reshape(128, -1)
    sels = sels.reshape(128, -1)
    xb = np.stack([np.stack([xc, -xs], 0), np.stack([xs, xc], 0)], 0)
    xb = xb.reshape(2, 2, KX, rows, a).transpose(3, 0, 4, 1, 2).reshape(rows * 2 * a, 2 * KX)
    xbh, xbl = np_halves(xb)
    xb3 = np.concatenate([xbh, xbh, xbl], 1)
    yb = np.stack([np.stack([yc, ys], 0), np.stack([-ys, yc], 0)], 0)
    yb = yb.reshape(2, 2, rows, kyl, cols, b).transpose(4, 3, 2, 0, 1, 5)
    yb = np.broadcast_to(yb[..., None, :], (cols, kyl, rows, 2, 2, a, b)).reshape(cols, kyl, rows * 2, 2 * cells)
    ybh, ybl = np_halves(yb)
    twice = np.where(np.arange(KZ) == 0, 1.0, 2.0)[:, None]
    zb = np.stack([twice * zc, -twice * zs], 0).reshape(2, cols, kzl, nz).transpose(1, 0, 2, 3).reshape(2 * KZ, nz)
    zbh, zbl = np_halves(zb)
    zb3 = np.concatenate([zbh, zbh, zbl], 0)
    yf = np.stack([yc, ys], 0).reshape(2, rows, kyl, 1, cols, 1, b)
    yf = (yf * np.eye(a).reshape(1, 1, 1, a, 1, a, 1)).reshape(2 * rows * kyl * a, cols * cells).T
    yfh, yfl = np_halves(yf)

    combined = jnp.dot(local_weight, lift_weight, precision=HIGHEST)
    offset = jnp.dot(local_weight, lift_bias, precision=HIGHEST) + local_bias
    origin = (lax.axis_index("row") == 0) & (lax.axis_index("col") == 0)
    last = np.arange(group * channels)[None, :] >= width_in * channels
    flag = jnp.where(jnp.asarray(last) & origin, 1.0, 0.0).astype(F32)

    results = []
    for sample in range(samples):
        vel = velocity[sample].reshape(width_in, cells, nz)
        tend = tendency[sample].reshape(width_in, cells, nz)
        step = step_size[sample].reshape(1)
        part = min(kzl, 4)
        chunks = kzl // part
        chunk_lanes = kyl * part * channels
        dma = lambda *shape: pltpu.SemaphoreType.DMA(shape)
        pencils_z = pl.pallas_call(
            functools.partial(layer_kernel, kyl, kzl, part, 1.0 / (full_x * full_y * nz)),
            out_shape=jax.ShapeDtypeStruct((cols, 2, kzl * channels, cells), F32),
            in_specs=[vmem, vmem, smem, vmem, vmem, vmem, pl.BlockSpec(memory_space=pl.ANY)] + [vmem] * 8,
            out_specs=vmem,
            scratch_shapes=[
                pltpu.VMEM(stored.shape, BF16),
                pltpu.VMEM((2 * modes, group * channels), F32),
                pltpu.VMEM((cols, width_in * rk, cells), F32),
                pltpu.VMEM((cols, width_in * rk, cells), F32),
                pltpu.VMEM((128, rows * kyl * a), F32),
                pltpu.VMEM((rows, kyl * a, 128), F32),
                pltpu.VMEM((rows, kyl * a, 128), F32),
                pltpu.VMEM((6 * KX, chunk_lanes), BF16),
                pltpu.VMEM((chunks, rows, 2 * a, chunk_lanes), F32),
                pltpu.VMEM((chunks, rows, 2 * a, chunk_lanes), F32),
                pltpu.VMEM((part * channels, 3 * kyl * rows * 2 * a), BF16),
                pltpu.VMEM((chunks, cols - 1, 2, part * channels, cells), F32),
                pltpu.SemaphoreType.DMA,
                dma(cols - 1), dma(cols - 1), dma(rows - 1), dma(rows - 1),
                dma(chunks, rows - 1), dma(chunks, rows - 1), dma(chunks, cols - 1), dma(chunks, cols - 1),
            ],
            compiler_params=pltpu.CompilerParams(
                vmem_limit_bytes=48 * 1024 * 1024, collective_id=0, has_side_effects=True
            ),
        )(
            vel, tend, step, jnp.asarray(zf), jnp.asarray(yfh), jnp.asarray(yfl), stored, lift_map, jnp.asarray(xf),
            jnp.asarray(selc, BF16), jnp.asarray(sels, BF16), flag, jnp.asarray(xb3), jnp.asarray(ybh), jnp.asarray(ybl),
        )
        pencils_z = pencils_z.reshape(cols * 2 * kzl * channels, cells)
        block = 4
        whole = lambda *shape: pl.BlockSpec(shape, lambda i: (0,) * len(shape))
        features = pl.pallas_call(
            functools.partial(z_back_kernel, channels, block),
            grid=(channels // block,),
            out_shape=jax.ShapeDtypeStruct((channels, cells, nz), BF16),
            in_specs=[
                whole(*pencils_z.shape), whole(width_in, cells, nz), whole(width_in, cells, nz),
                smem, smem, smem, whole(*zb3.shape),
            ],
            out_specs=pl.BlockSpec((block, cells, nz), lambda i: (i, 0, 0)),
            scratch_shapes=[pltpu.VMEM((width_in, cells, nz), F32)],
            compiler_params=big,
        )(
            pencils_z, vel, tend, step, combined, offset, jnp.asarray(zb3),
        )
        results.append(features.reshape(channels, a, b, nz))
    return jnp.stack(results, 0)


def solution(mesh):
    in_specs = (
        P(None, None, "row", "col", None),
        P(None, None, "row", "col", None),
        P(),
        P(),
        P(),
        P(None, "row", "col", None, None),
        P(),
        P(),
    )
    out_specs = P(None, None, "row", "col", None)
    return jax.shard_map(
        per_device, mesh=mesh, in_specs=in_specs, out_specs=out_specs, check_vma=False
    )
```

```python
import functools
import math

import jax
import jax.numpy as jnp
import numpy as np
from jax import lax
from jax.experimental import pallas as pl
from jax.experimental.pallas import tpu as pltpu
from jax.sharding import PartitionSpec as P

KX = 32
KY = 32
KZ = 32
HIGHEST = lax.Precision.HIGHEST
F32 = jnp.float32
BF16 = jnp.bfloat16


def waves(count):
    index = np.arange(count)
    return np.where(index < count // 2, index, index - count)


def trig(wave, length):
    angle = ((wave[:, None] * np.arange(length)[None, :]) % length) * (2.0 * math.pi / length)
    return np.cos(angle), np.sin(angle)


def np_halves(table):
    table = np.asarray(table, np.float32)
    high = table.astype(jnp.bfloat16)
    low = (table - high.astype(np.float32)).astype(jnp.bfloat16)
    return high, low


def split(x):
    high = x.astype(BF16)
    return high, (x - high.astype(F32)).astype(BF16)


def dot(a, b):
    return jnp.dot(a, b, preferred_element_type=F32)


MESH = pl.DeviceIdType.MESH


def column(line):
    n = line.shape[1]
    own = lax.broadcasted_iota(jnp.int32, (n, n), 0) == lax.broadcasted_iota(jnp.int32, (n, n), 1)
    return jnp.sum(jnp.where(own, line, 0.0), axis=1, keepdims=True)


def layer_kernel(
    kyl, kzl, part, scale, vel_ref, tend_ref, step_ref, zf_ref, yfh_ref, yfl_ref, w_ref, lw_ref, lb_ref, xf_ref, selc_ref,
    sels_ref, xb_ref, yh_ref, yl_ref, out_ref, lift_ref, w_vmem, wl_ref, zsend, zrecv, ypad, ysend, yrecv, m_ref, xsend, xrecv,
    lhs_ref, csend, w_sem, z_ss, z_rs, y_ss, y_rs, x_ss, x_rs, c_ss, c_rs,
):
    rows, cols = lax.axis_size("row"), lax.axis_size("col")
    my_row, my_col = lax.axis_index("row"), lax.axis_index("col")
    width_in, cells, _ = vel_ref.shape
    rk = zf_ref.shape[0] // cols
    a = ysend.shape[1] // kyl
    b = cells // a
    modes = kyl * kzl * KX
    chunks = xsend.shape[0]

    load = pltpu.make_async_copy(w_ref, w_vmem, w_sem)
    load.start()
    barrier = pltpu.get_barrier_semaphore()
    row_peers = [lax.rem(my_row + i, rows) for i in range(1, rows)]
    col_peers = [lax.rem(my_col + i, cols) for i in range(1, cols)]
    for peer in row_peers:
        pl.semaphore_signal(barrier, inc=1, device_id={"row": peer}, device_id_type=MESH)
    for peer in col_peers:
        pl.semaphore_signal(barrier, inc=1, device_id={"col": peer}, device_id_type=MESH)

    for j in range(width_in):
        adv = vel_ref[j] + step_ref[0] * tend_ref[j]
        z = lax.dot_general(
            zf_ref[...], adv, (((1,), (1,)), ((), ())), precision=HIGHEST, preferred_element_type=F32
        )
        zsend[:, j * rk:(j + 1) * rk, :] = z.reshape(cols, rk, cells)
    pl.semaphore_wait(barrier, rows + cols - 2)
    z_copies = []
    for i, peer in enumerate(col_peers):
        copy = pltpu.make_async_remote_copy(
            zsend.at[peer], zrecv.at[my_col], z_ss.at[i], z_rs.at[i], device_id={"col": peer}, device_id_type=MESH
        )
        copy.start()
        z_copies.append(copy)
    zrecv[pl.ds(my_col, 1)] = zsend[pl.ds(my_col, 1)]

    channels = lb_ref.shape[1]
    place = lax.broadcasted_iota(jnp.int32, (channels, 128), 1)
    base = jnp.broadcast_to(column(lb_ref[...]), (channels, 128))
    for j in range(width_in):
        base = jnp.where(place // channels == j, column(lw_ref[j:j + 1, :]), base)
    for o in range(channels):
        lh, ll = split(jnp.where(place % channels == o, base, 0.0))
        lift_ref[o * channels:(o + 1) * channels, :128] = lh
        lift_ref[o * channels:(o + 1) * channels, 128:] = ll

    load.wait()
    step_rows = modes // 2
    half_lanes = lift_ref.shape[1] // 2

    def weigh(n):
        at = slice(n * step_rows, (n + 1) * step_rows)
        both = dot(w_vmem[at, :], lift_ref[...])
        wl_ref[at, :] = both[:, :half_lanes] + both[:, half_lanes:]

    weigh(0)
    weigh(1)
    for copy in z_copies:
        copy.wait_recv()

    x = jnp.concatenate([zrecv[s] for s in range(cols)], 1)
    xh, xl = split(x)
    y = dot(xh, yfh_ref[...]) + dot(xl, yfh_ref[...]) + dot(xh, yfl_ref[...])
    lanes = rows * kyl * a
    ypad[...] = jnp.zeros_like(ypad)
    low_rows = lax.broadcasted_iota(jnp.int32, (rk, lanes), 0) < rk // 2
    for j in range(width_in):
        block = y[j * rk:(j + 1) * rk]
        turned = pltpu.roll(block[:, lanes:], rk // 2, 0)
        ypad[j * rk:(j + 1) * rk, :] = block[:, :lanes] + jnp.where(low_rows, turned, -turned)
    ysend[...] = jnp.transpose(ypad[...]).reshape(ysend.shape)
    y_copies = []
    for i, peer in enumerate(row_peers):
        copy = pltpu.make_async_remote_copy(
            ysend.at[peer], yrecv.at[my_row], y_ss.at[i], y_rs.at[i], device_id={"row": peer}, device_id_type=MESH
        )
        copy.start()
        y_copies.append(copy)
    yrecv[pl.ds(my_row, 1)] = ysend[pl.ds(my_row, 1)]
    weigh(2)
    weigh(3)
    for copy in y_copies:
        copy.wait_recv()

    cos_parts, sin_parts = [], []
    for l in range(kyl):
        u = yrecv[:, l * a:(l + 1) * a, :].reshape(rows * a, yrecv.shape[2])
        q = jnp.dot(xf_ref[...], u, precision=HIGHEST, preferred_element_type=F32) * scale
        cos_parts.append(q[:KX])
        sin_parts.append(q[KX:])
    ch, cl = split(jnp.concatenate(cos_parts, 0))
    sh, sl = split(jnp.concatenate(sin_parts, 0))
    selc, sels = selc_ref[...], sels_ref[...]
    amp = dot(ch, selc) + dot(cl, selc) + dot(sh, sels) + dot(sl, sels)
    lane = lax.broadcasted_iota(jnp.int32, (KX, 128), 1)
    row = lax.broadcasted_iota(jnp.int32, (KX, 128), 0)
    quarter = lane // 32
    origin = jnp.where((my_row == 0) & (my_col == 0), 1.0, 0.0).astype(F32)
    order = [(l, c * part + k) for c in range(chunks) for l in range(kyl) for k in range(part)]
    chunk_lanes = xsend.shape[3]
    x_copies = []
    for c in range(chunks):
        for group in range(chunk_lanes // 128):
            packed_r = packed_i = None
            for q in range(4):
                l, k = order[(c * chunk_lanes // 128 + group) * 4 + q]
                ar = amp[l * KX:(l + 1) * KX, k * 256:k * 256 + 128]
                ai = amp[l * KX:(l + 1) * KX, k * 256 + 128:k * 256 + 256]
                if l == 0 and k == 0:
                    ar = ar + jnp.where((row == 0) & (lane >= width_in * channels), origin, 0.0)
                at = (l * kzl + k) * KX
                wr = wl_ref[at:at + KX, :]
                wi = wl_ref[modes + at:modes + at + KX, :]
                pr = wr * ar - wi * ai
                pi = wr * ai + wi * ar
                pr = pr + pltpu.roll(pr, 64, 1)
                pi = pi + pltpu.roll(pi, 64, 1)
                pr = pr + pltpu.roll(pr, 32, 1)
                pi = pi + pltpu.roll(pi, 32, 1)
                packed_r = pr if q == 0 else jnp.where(quarter == q, pr, packed_r)
                packed_i = pi if q == 0 else jnp.where(quarter == q, pi, packed_i)
            at = slice(group * 128, (group + 1) * 128)
            mh, ml = split(jnp.concatenate([packed_r, packed_i], 0))
            m_ref[0:2 * KX, at] = mh
            m_ref[2 * KX:4 * KX, at] = ml
            m_ref[4 * KX:6 * KX, at] = mh
        xsend[c] = dot(xb_ref[...], m_ref[...]).reshape(xsend.shape[1:])
        started = []
        for i, peer in enumerate(row_peers):
            copy = pltpu.make_async_remote_copy(
                xsend.at[c, peer], xrecv.at[c, my_row], x_ss.at[c, i], x_rs.at[c, i],
                device_id={"row": peer}, device_id_type=MESH,
            )
            copy.start()
            started.append(copy)
        xrecv[c, pl.ds(my_row, 1)] = xsend[c, pl.ds(my_row, 1)]
        x_copies.append(started)

    total = rows * 2 * a
    ko = chunk_lanes // kyl
    pairs = 2 * rows
    width = 2 * cells
    xr = lax.broadcasted_iota(jnp.int32, (pairs, a, width), 1)
    xl = (lax.broadcasted_iota(jnp.int32, (pairs, a, width), 2) // b) % a
    same = xr == xl

    def expand(table):
        full = jnp.where(same, table.astype(F32)[:, None, :], 0.0)
        return full.reshape(total, width).astype(BF16)

    c_copies = []
    for c in range(chunks):
        for copy in x_copies[c]:
            copy.wait_recv()
        for l in range(kyl):
            held = xrecv[c, :, :, l * ko:(l + 1) * ko].reshape(total, ko)
            th, tl = split(jnp.transpose(held))
            lhs_ref[:, l * total:(l + 1) * total] = th
            lhs_ref[:, (kyl + l) * total:(kyl + l + 1) * total] = tl
            lhs_ref[:, (2 * kyl + l) * total:(2 * kyl + l + 1) * total] = th
        at = pl.ds(c * ko, ko)
        for i in list(range(1, cols)) + [0]:
            d = lax.rem(my_col + i, cols)
            high = [expand(yh_ref[d, l]) for l in range(kyl)]
            low = [expand(yl_ref[d, l]) for l in range(kyl)]
            acc = dot(lhs_ref[...], jnp.concatenate(high + high + low, 0))
            if i == 0:
                for v in range(2):
                    out_ref[pl.ds(my_col, 1), v, at, :] = acc[:, v * cells:(v + 1) * cells][None]
            else:
                for v in range(2):
                    csend[c, i - 1, v] = acc[:, v * cells:(v + 1) * cells]
                copy = pltpu.make_async_remote_copy(
                    csend.at[c, i - 1], out_ref.at[my_col, :, at, :], c_ss.at[c, i - 1], c_rs.at[c, i - 1],
                    device_id={"col": d}, device_id_type=MESH,
                )
                copy.start()
                c_copies.append(copy)
    for copy in c_copies:
        copy.wait_recv()
    for copy in z_copies + y_copies + [copy for started in x_copies for copy in started] + c_copies:
        copy.wait_send()


def z_back_kernel(channels, block, d_ref, vel_ref, tend_ref, step_ref, lw_ref, lb_ref, mw_ref, mb_ref, tz_ref, out_ref, adv_ref, line_ref):
    first = pl.program_id(0)
    depth = d_ref.shape[0] // channels

    @pl.when(first == 0)
    def _():
        adv_ref[...] = vel_ref[...] + step_ref[0] * tend_ref[...]
        width_in = lw_ref.shape[0]
        for j in range(width_in + 1):
            line = lw_ref[j:j + 1, :] if j < width_in else lb_ref[...]
            wide = jnp.broadcast_to(column(line), (channels, line_ref.shape[2]))
            mapped = jnp.dot(mw_ref[...], wide, precision=HIGHEST, preferred_element_type=F32)
            line_ref[j] = mapped if j < width_in else mapped + column(mb_ref[...])

    for i in range(block):
        o = first * block + i
        high, low = split(d_ref[pl.ds(o, depth, stride=channels), :])
        lhs = jnp.concatenate([high, low, high], 0)
        spectral = lax.dot_general(lhs, tz_ref[...], (((0,), (0,)), ((), ())), preferred_element_type=F32)
        x = spectral + line_ref[adv_ref.shape[0], pl.ds(o, 1), :]
        for j in range(adv_ref.shape[0]):
            x = x + line_ref[j, pl.ds(o, 1), :] * adv_ref[j]
        inner = x * (0.7978845608028654 + 0.035677408136300125 * (x * x))
        half = 0.5 * x
        out_ref[i] = (half + half * jnp.tanh(inner)).astype(BF16)


def per_device(
    velocity, tendency, step_size, lift_weight, lift_bias, spectral_weight, local_weight, local_bias
):
    samples, width_in, a, b, nz = velocity.shape
    channels = lift_weight.shape[0]
    rows, cols = lax.axis_size("row"), lax.axis_size("col")
    full_x, full_y = a * rows, b * cols
    kzl, kyl = KZ // cols, KY // rows
    modes = kyl * kzl * KX
    cells = a * b
    vmem = pl.BlockSpec(memory_space=pltpu.VMEM)
    smem = pl.BlockSpec(memory_space=pltpu.SMEM)
    big = pltpu.CompilerParams(vmem_limit_bytes=48 * 1024 * 1024)

    group = width_in + 1
    stored = spectral_weight.reshape(2 * modes, channels * channels)

    zc, zs = trig(np.arange(KZ), nz)
    rk = 2 * max(kzl, 4)
    zf = np.zeros((cols, 2, rk // 2, nz), np.float32)
    zf[:, :, :kzl] = np.stack([zc, -zs], 0).reshape(2, cols, kzl, nz).transpose(1, 0, 2, 3)
    zf = zf.reshape(cols * rk, nz)
    yc, ys = trig(waves(KY), full_y)
    xc, xs = trig(waves(KX), full_x)
    xf = np.concatenate([xc, xs], 0).astype(np.float32)
    selc = np.zeros((128, kzl, 2, group, channels), np.float32)
    sels = np.zeros_like(selc)
    for j in range(width_in):
        for k in range(kzl):
            re, im = j * rk + k, j * rk + rk // 2 + k
            selc[re, k, 0, j] = 1
            selc[im, k, 1, j] = 1
            sels[im, k, 0, j] = 1
            sels[re, k, 1, j] = -1
    selc = selc.reshape(128, -1)
    sels = sels.reshape(128, -1)
    xb = np.stack([np.stack([xc, -xs], 0), np.stack([xs, xc], 0)], 0)
    xb = xb.reshape(2, 2, KX, rows, a).transpose(3, 0, 4, 1, 2).reshape(rows * 2 * a, 2 * KX)
    xbh, xbl = np_halves(xb)
    xb3 = np.concatenate([xbh, xbh, xbl], 1)
    yb = np.stack([np.stack([yc, ys], 0), np.stack([-ys, yc], 0)], 0)
    yb = yb.reshape(2, 2, rows, kyl, cols, b).transpose(4, 3, 2, 0, 1, 5)
    yb = np.broadcast_to(yb[..., None, :], (cols, kyl, rows, 2, 2, a, b)).reshape(cols, kyl, rows * 2, 2 * cells)
    ybh, ybl = np_halves(yb)
    twice = np.where(np.arange(KZ) == 0, 1.0, 2.0)[:, None]
    zb = np.stack([twice * zc, -twice * zs], 0).reshape(2, cols, kzl, nz).transpose(1, 0, 2, 3).reshape(2 * KZ, nz)
    zbh, zbl = np_halves(zb)
    zb3 = np.concatenate([zbh, zbh, zbl], 0)
    yf = np.stack([yc, ys], 0).reshape(2, rows, kyl, 1, cols, 1, b)
    yf = (yf * np.eye(a).reshape(1, 1, 1, a, 1, a, 1)).reshape(2 * rows * kyl * a, cols * cells).T
    yfh, yfl = np_halves(yf)

    results = []
    for sample in range(samples):
        vel = velocity[sample].reshape(width_in, cells, nz)
        tend = tendency[sample].reshape(width_in, cells, nz)
        step = step_size[sample].reshape(1)
        part = min(kzl, 4)
        chunks = kzl // part
        chunk_lanes = kyl * part * channels
        dma = lambda *shape: pltpu.SemaphoreType.DMA(shape)
        pencils_z = pl.pallas_call(
            functools.partial(layer_kernel, kyl, kzl, part, 1.0 / (full_x * full_y * nz)),
            out_shape=jax.ShapeDtypeStruct((cols, 2, kzl * channels, cells), F32),
            in_specs=[vmem, vmem, smem, vmem, vmem, vmem, pl.BlockSpec(memory_space=pl.ANY)] + [vmem] * 8,
            out_specs=vmem,
            scratch_shapes=[
                pltpu.VMEM((channels * channels, 2 * group * channels), BF16),
                pltpu.VMEM(stored.shape, BF16),
                pltpu.VMEM((2 * modes, group * channels), F32),
                pltpu.VMEM((cols, width_in * rk, cells), F32),
                pltpu.VMEM((cols, width_in * rk, cells), F32),
                pltpu.VMEM((128, rows * kyl * a), F32),
                pltpu.VMEM((rows, kyl * a, 128), F32),
                pltpu.VMEM((rows, kyl * a, 128), F32),
                pltpu.VMEM((6 * KX, chunk_lanes), BF16),
                pltpu.VMEM((chunks, rows, 2 * a, chunk_lanes), F32),
                pltpu.VMEM((chunks, rows, 2 * a, chunk_lanes), F32),
                pltpu.VMEM((part * channels, 3 * kyl * rows * 2 * a), BF16),
                pltpu.VMEM((chunks, cols - 1, 2, part * channels, cells), F32),
                pltpu.SemaphoreType.DMA,
                dma(cols - 1), dma(cols - 1), dma(rows - 1), dma(rows - 1),
                dma(chunks, rows - 1), dma(chunks, rows - 1), dma(chunks, cols - 1), dma(chunks, cols - 1),
            ],
            compiler_params=pltpu.CompilerParams(
                vmem_limit_bytes=48 * 1024 * 1024, collective_id=0, has_side_effects=True
            ),
        )(
            vel, tend, step, jnp.asarray(zf), jnp.asarray(yfh), jnp.asarray(yfl), stored, lift_weight.T, lift_bias[None],
            jnp.asarray(xf),
            jnp.asarray(selc, BF16), jnp.asarray(sels, BF16), jnp.asarray(xb3), jnp.asarray(ybh), jnp.asarray(ybl),
        )
        pencils_z = pencils_z.reshape(cols * 2 * kzl * channels, cells)
        block = 4
        whole = lambda *shape: pl.BlockSpec(shape, lambda i: (0,) * len(shape))
        features = pl.pallas_call(
            functools.partial(z_back_kernel, channels, block),
            grid=(channels // block,),
            out_shape=jax.ShapeDtypeStruct((channels, cells, nz), BF16),
            in_specs=[
                whole(*pencils_z.shape), whole(width_in, cells, nz), whole(width_in, cells, nz),
                smem, vmem, vmem, vmem, vmem, whole(*zb3.shape),
            ],
            out_specs=pl.BlockSpec((block, cells, nz), lambda i: (i, 0, 0)),
            scratch_shapes=[pltpu.VMEM((width_in, cells, nz), F32), pltpu.VMEM((group, channels, nz), F32)],
            compiler_params=big,
        )(
            pencils_z, vel, tend, step, lift_weight.T, lift_bias[None], local_weight, local_bias[None], jnp.asarray(zb3),
        )
        results.append(features.reshape(channels, a, b, nz))
    return jnp.stack(results, 0)


def solution(mesh):
    in_specs = (
        P(None, None, "row", "col", None),
        P(None, None, "row", "col", None),
        P(),
        P(),
        P(),
        P(None, "row", "col", None, None),
        P(),
        P(),
    )
    out_specs = P(None, None, "row", "col", None)
    return jax.shard_map(
        per_device, mesh=mesh, in_specs=in_specs, out_specs=out_specs, check_vma=False
    )
```
